32 devices in a mesh: section: 4 (over x, core), shard: 2 (over y), replica: 4 (over z).
Axes of the slice: x: 2, y: 2, z: 4, core: 2. Of those that a mesh axis runs over, the one named last changes fastest.
Arguments:
- acts_fwd: bfloat16 [4, 1024, 4096], P('section', ('shard', 'replica')), may hold values from -30 to 30
- pos_fwd: int32 [4, 1024], P('section', ('shard', 'replica')), may hold values from 0 to 2047
- saved_acts: bfloat16 [4, 1024, 4096], P('section', ('shard', 'replica')), may hold values from -30 to 30
- pos_bwd: int32 [4, 1024], P('section', ('shard', 'replica')), may hold values from 0 to 2047
- grads_in: bfloat16 [4, 1024, 4096], P('section', ('shard', 'replica')), may hold values from -6 to 6
- key_cotan: bfloat16 [4, 1024, 512], P('section', ('shard', 'replica')), may hold values from -6 to 6
- weight: bfloat16 [4, 4096, 512], P('section', 'shard'), may hold values from -0.09375 to 0.09375
- gain: float32 [4, 4096], P('section'), may hold values from 0.1 to 1.9
Outputs:
- keys: bfloat16 [4, 1024, 512], P('section', ('shard', 'replica'))
- grad_out: bfloat16 [4, 1024, 4096], P('section', ('shard', 'replica'))
- weight_grad: float32 [4, 4096, 512], P('section', 'shard')
The draws below stay inside these ranges and needn't reach their ends.
All inputs are finite; a program needn't handle non-finite values.
Results may differ from the reference program's by a relative error of at most 0.0058.
Values may be sent and summed in bfloat16 or wider, within the bound.
A program may use at most 64 MiB of HBM per device.

```python
import math
import jax
import jax.numpy as jnp
from jax import lax

D = 4096
HEAD = 128
KVH = 4
SEQ = 2048
TOK_DEV = 128
TOKENS = 1024
N_SECTION = 4


def rough_rows(key):
    shape = (N_SECTION, TOKENS, D)
    scale_key = jax.random.fold_in(key, 11)
    base_key = jax.random.fold_in(key, 12)
    scales = jnp.exp(jax.random.uniform(scale_key, (N_SECTION, TOKENS, 1), jnp.float32, math.log(0.5), math.log(5.0)))
    base = jnp.clip(jax.random.normal(base_key, shape, jnp.float32), -5.0, 5.0)
    values = base * scales
    return jnp.clip(values, -30.0, 30.0).astype(jnp.bfloat16)


def draw_acts_fwd(key, part):
    return rough_rows(jax.random.fold_in(key, 101))


def draw_saved_acts(key, part):
    return rough_rows(jax.random.fold_in(key, 202))


def plant(entries, own_key, smallest, top_value):
    shape = entries.shape
    index_at = [jax.random.randint(jax.random.fold_in(own_key, axis), (), 0, shape[axis]) for axis in range(len(shape))]
    entries = entries.at[tuple(index_at)].set(smallest)
    longest = shape.index(max(shape))
    index_at[longest] = (index_at[longest] + 1) % shape[longest]
    return entries.at[tuple(index_at)].set(top_value)


def levels(key, shape, pieces, low, largest):
    def one(axis_at, shards_of):
        heights = jax.random.uniform(jax.random.fold_in(jax.random.fold_in(key, 6), axis_at), (shards_of,), jnp.float32, low / len(pieces), largest / len(pieces))
        return jnp.repeat(jnp.exp(heights), shape[axis_at] // shards_of).reshape((-1,) + (1,) * (len(shape) - axis_at - 1))

    factor_of = one(*pieces[0])
    for cut in pieces[1:]:
        factor_of = factor_of * one(*cut)
    return factor_of


def noise(own_key, extent, width, limit, split=(), kind=jnp.bfloat16):
    values = width * jax.random.normal(own_key, extent, jnp.float32)
    if split:
        values = values * levels(own_key, extent, split, -0.22, 0.18)
    return jnp.clip(values, -limit, limit).astype(kind)


def setup_inputs(seed: int = 0) -> dict:
    key_list = jax.random.split(jax.random.key(seed), 9)
    acts_fwd = draw_acts_fwd(jax.random.fold_in(key_list[8], 71), 0)
    pos_fwd = plant(jax.random.randint(key_list[1], (N_SECTION, TOKENS), 0, SEQ), jax.random.fold_in(key_list[1], 1), 0, SEQ - 1).astype(jnp.int32)
    saved_acts = draw_saved_acts(jax.random.fold_in(key_list[8], 71), 0)
    pos_bwd = plant(jax.random.randint(key_list[3], (N_SECTION, TOKENS), 0, SEQ), jax.random.fold_in(key_list[3], 1), 0, SEQ - 1).astype(jnp.int32)
    grads_in = noise(key_list[4], (N_SECTION, TOKENS, D), 1.0, 6.0, ((0, 4), (1, 8)))
    key_cotan = noise(key_list[5], (N_SECTION, TOKENS, KVH * HEAD), 1.0, 6.0, ((0, 4), (1, 8)))
    weight = noise(key_list[6], (N_SECTION, D, KVH * HEAD), D ** -0.5, 0.09375, ((0, 4), (1, 2)))
    gain = jnp.clip(1.0 + 0.18 * jax.random.normal(key_list[7], (N_SECTION, D), jnp.float32), 0.1, 1.9)
    return dict(acts_fwd=acts_fwd, pos_fwd=pos_fwd, saved_acts=saved_acts, pos_bwd=pos_bwd, grads_in=grads_in, key_cotan=key_cotan, weight=weight, gain=gain)


def rope_tables(positions):
    index = jnp.arange(HEAD // 2, dtype=jnp.float32)
    rate = 500000.0 ** (-(2.0 * index) / HEAD)
    angle = positions.astype(jnp.float32)[:, None] * rate[None, :]
    return (jnp.cos(angle), jnp.sin(angle))

def rotate(values, cosine, sine_part, orient):
    count = values.shape[0]
    shaped = values.reshape(count, KVH, HEAD)
    first_half = shaped[..., :HEAD // 2]
    second_half = shaped[..., HEAD // 2:]
    cos_b = cosine[:, None, :]
    sin_b = orient * sine_part[:, None, :]
    joined = jnp.concatenate([first_half * cos_b - second_half * sin_b, second_half * cos_b + first_half * sin_b], -1)
    return joined.reshape(count, KVH * HEAD)

def normalize(stream, gain_row):
    values = stream.astype(jnp.float32)
    inverse = lax.rsqrt(lax.optimization_barrier(jnp.mean(values * values, -1, keepdims=True)) + 1e-05)
    return (values * inverse * gain_row[None, :], inverse, values)

def one_section(packed):
    stream, pos_f, saved, pos_b, arrived, cotan, proj, gain_row = packed
    normed = normalize(stream, gain_row)[0].astype(jnp.bfloat16)
    projected = jnp.dot(normed, proj, preferred_element_type=jnp.float32)
    cosine, sine_part = rope_tables(pos_f)
    keys = rotate(projected, cosine, sine_part, 1.0).astype(jnp.bfloat16)
    back_f, inverse, saved_f = normalize(saved, gain_row)
    back_normed = back_f.astype(jnp.bfloat16)
    cos_b, sin_b = rope_tables(pos_b)
    key_grad = rotate(cotan.astype(jnp.float32), cos_b, sin_b, -1.0).astype(jnp.bfloat16)
    normed_grad = jnp.dot(key_grad, proj.T, preferred_element_type=jnp.float32)
    scaled = normed_grad * gain_row[None, :]
    stream_grad = inverse * scaled - saved_f * inverse ** 3 * lax.optimization_barrier(jnp.mean(saved_f * scaled, -1, keepdims=True))
    grad_out = (arrived.astype(jnp.float32) + stream_grad).astype(jnp.bfloat16)
    blocks = TOKENS // TOK_DEV
    norm_blocks = back_normed.reshape(blocks, TOK_DEV, D)
    grad_blocks = key_grad.reshape(blocks, TOK_DEV, KVH * HEAD)

    def accumulate(total, pair):
        term = lax.dot_general(pair[0], pair[1], (((0,), (0,)), ((), ())), preferred_element_type=jnp.float32)
        rounded = lax.optimization_barrier(term.astype(jnp.bfloat16))
        return (total + rounded.astype(jnp.float32), None)
    start = jnp.zeros((D, KVH * HEAD), jnp.float32)
    total, unused = lax.scan(accumulate, start, (norm_blocks, grad_blocks))
    weight_grad = total * float(TOKENS) ** (-0.5)
    return (keys, grad_out, weight_grad)

def reference(acts_fwd, pos_fwd, saved_acts, pos_bwd, grads_in, key_cotan, weight, gain):
    streams = jnp.concatenate([acts_fwd[:1], acts_fwd[:-1]], 0)
    arrivals = jnp.concatenate([grads_in[1:], grads_in[-1:]], 0)
    keys, grad_out, weight_grad = lax.map(one_section, (streams, pos_fwd, saved_acts, pos_bwd, arrivals, key_cotan, weight, gain))
    return (keys, grad_out, weight_grad)
```

```python
import functools

import jax
import jax.numpy as jnp
import numpy as np
from jax import lax
from jax.experimental import pallas as pl
from jax.experimental.pallas import tpu as pltpu
from jax.sharding import PartitionSpec as P

HEAD = 128
THETA = 500000.0
EPS = 1e-05
ROWS = 128
PARTS = 4
RIGHT = 6
LEFT = 4
LOADS = 2
SENDS = 8
CUTS = 4
SPAN = 64
PLAN = dict(relay=6, backward=8, own=14, peers=36, means=50, grads=54, keys=60)
F32 = jnp.float32
BF16 = jnp.bfloat16
MESH = pl.DeviceIdType.MESH


def sine_cosine(angle):
    turn = jnp.floor(angle * (2.0 / np.pi) + 0.5)
    x = angle - turn * 1.5703125
    x = x - turn * 4.837512969970703125e-4
    x = x - turn * 7.54978995489188216e-8
    y = x * x
    s = ((-1.9515295891e-4 * y + 8.3321608736e-3) * y - 1.6666654611e-1) * y * x + x
    c = (2.443315711809948e-5 * y - 1.388731625493765e-3) * y + 4.166664568298827e-2
    c = c * y * y - 0.5 * y + 1.0
    quarter = turn.astype(jnp.int32) & 3
    odd = (quarter & 1) == 1
    sine, cosine = jnp.where(odd, c, s), jnp.where(odd, s, c)
    sine = jnp.where(quarter >= 2, -sine, sine)
    cosine = jnp.where((quarter == 1) | (quarter == 2), -cosine, cosine)
    return sine, cosine


def pieces_of(blocks):
    pieces, at = [], 0
    while at < blocks:
        size = min(max(at, 1), blocks - at)
        pieces.append((at, size))
        at += size
    return pieces


def rings(C, R):
    ring = min(C, max(RIGHT, LEFT) * (R - 1) + 2)
    return min(C, SENDS), ring, ring


def kernel(
    X, S, R,
    acts, grads, saved, kcot, w, gain_h, pos_f, pos_b, rate_h,
    keys_o, grad_o, wg_o,
    saved_v, kcot_v, w_v, stream_v, arrived_v, gain, posf_v, posb_v, rate,
    sv_recv, kg_all, st_recv, g_buf, g_send, p_buf, p_send, p_acc,
    part, from_l, from_r, to_r, to_l, inv_all, inv_row, tab_v, sum_v, first,
    lsem, saved_sem, acts_ss, acts_rs, grads_sem, sv_ss, sv_rs, kg_ss, kg_rs, iv_ss, iv_rs,
    st_ss, st_rs, g_ss, g_rs, p_ss, p_rs, r_ss, r_rs, l_ss, l_rs,
):
    s, j, r = (lax.axis_index(a) for a in ("section", "shard", "replica"))
    T, D = saved.shape
    N = kcot.shape[1]
    Fs = w.shape[0]
    blocks = Fs // ROWS
    C = blocks * PARTS
    width = N // PARTS
    tile = min(512, Fs)
    tiles = Fs // tile
    wide = min(1024, Fs)
    spans = D // wide
    travel = to_r.dtype
    pieces = pieces_of(blocks)
    sends, right_ring, left_ring = rings(C, R)
    cut = ROWS // CUTS

    barrier = pltpu.get_barrier_semaphore()

    def greet(axis, index):
        pl.semaphore_signal(barrier, inc=1, device_id={axis: index}, device_id_type=MESH)

    def cols(p, width=Fs, off=0):
        return pl.ds(pl.multiple_of(p * Fs + off, 128), width)

    def peer(d):
        return lax.rem(j + d, S)

    for d in range(1, S):
        greet("shard", peer(d))
    pl.when(r > 0)(lambda: greet("replica", r - 1))
    pl.when(r < R - 1)(lambda: greet("replica", r + 1))
    pl.when(s > 0)(lambda: greet("section", s - 1))
    pl.when(s < X - 1)(lambda: greet("section", s + 1))

    load_kcot = pltpu.make_async_copy(kcot, kcot_v, lsem.at[0])
    load_w = pltpu.make_async_copy(w, w_v, lsem.at[0])
    load_acts = pltpu.make_async_copy(acts, stream_v, lsem.at[1])
    load_grads = pltpu.make_async_copy(grads, arrived_v, lsem.at[2])
    load_posb = pltpu.make_async_copy(pos_b, posb_v, lsem.at[1])
    load_posf = pltpu.make_async_copy(pos_f, posf_v, lsem.at[3])
    load_rate = pltpu.make_async_copy(rate_h, rate, lsem.at[2])
    load_gain = pltpu.make_async_copy(gain_h, gain, lsem.at[4])
    Dl = D // LOADS
    load_saved = [
        pltpu.make_async_copy(
            saved.at[:, pl.ds(i * Dl, Dl)], saved_v.at[:, pl.ds(i * Dl, Dl)], saved_sem.at[i]
        )
        for i in range(LOADS)
    ]
    load_posb.start()
    load_rate.start()
    load_kcot.start()
    for copy in load_saved:
        copy.start()
    load_gain.start()
    load_posf.start()

    def remote(src, dst, ss, rs, axis, index):
        return pltpu.make_async_remote_copy(
            src_ref=src, dst_ref=dst, send_sem=ss, recv_sem=rs,
            device_id={axis: index}, device_id_type=MESH,
        )

    def shard_copy(src, dst, ss, rs, d, *index):
        return remote(
            src, dst, ss.at[(d - 1, *index)], rs.at[(S - d - 1, *index)], "shard", peer(d)
        )

    def shard_wait(src, dst, ss, rs, slot, *index):
        remote(
            src, dst, ss.at[(slot - 1, *index)], rs.at[(slot - 1, *index)], "shard", peer(slot)
        ).wait_recv()

    def sv_copy(d, q):
        at, size = (v * ROWS for v in pieces[q])
        return shard_copy(
            saved_v.at[:, cols(peer(d), size, at)], sv_recv.at[S - d, :, pl.ds(at, size)],
            sv_ss, sv_rs, d, q,
        )

    def sv_wait(slot, q):
        at, size = (v * ROWS for v in pieces[q])
        shard_wait(
            saved_v.at[:, pl.ds(0, size)], sv_recv.at[slot, :, pl.ds(at, size)],
            sv_ss, sv_rs, slot, q,
        )

    def kg_copy(d, h):
        at = pl.ds(h * width, width)
        return shard_copy(kg_all.at[0, :, at], kg_all.at[S - d, :, at], kg_ss, kg_rs, d, h)

    def kg_wait(slot, h):
        at = pl.ds(h * width, width)
        shard_wait(kg_all.at[0, :, at], kg_all.at[slot, :, at], kg_ss, kg_rs, slot, h)

    def iv_copy(d):
        return shard_copy(inv_row.at[0], inv_row.at[S - d], iv_ss, iv_rs, d)

    def iv_wait(slot):
        shard_wait(inv_row.at[0], inv_row.at[slot], iv_ss, iv_rs, slot)

    def p_copy(d):
        return shard_copy(p_send.at[d], p_buf.at[S - d], p_ss, p_rs, d)

    def p_wait(slot):
        shard_wait(p_send.at[slot], p_buf.at[slot], p_ss, p_rs, slot)

    def g_copy(d, i):
        at = pl.ds(pl.multiple_of(i * tile, 128), tile)
        return shard_copy(g_send.at[d, :, at], g_buf.at[S - d, :, at], g_ss, g_rs, d, i)

    def g_wait(slot, i):
        at = pl.ds(pl.multiple_of(i * tile, 128), tile)
        shard_wait(g_send.at[slot, :, at], g_buf.at[slot, :, at], g_ss, g_rs, slot, i)

    def acts_copy(d):
        return remote(
            acts.at[:, cols(peer(d))], stream_v.at[:, cols(peer(d))],
            acts_ss.at[d], acts_rs.at[d], "section", jnp.minimum(s + 1, X - 1),
        )

    grads_copy = remote(
        grads, arrived_v, grads_sem.at[0], grads_sem.at[1], "section", jnp.maximum(s - 1, 0)
    )

    def st_copy(d):
        return shard_copy(stream_v.at[:, cols(peer(d))], st_recv.at[S - d], st_ss, st_rs, d)

    def st_wait(slot):
        shard_wait(stream_v.at[:, pl.ds(0, Fs)], st_recv.at[slot], st_ss, st_rs, slot)

    def right_copy(c):
        return remote(
            to_r.at[c], from_l.at[c], r_ss.at[lax.rem(c, sends)], r_rs.at[lax.rem(c, right_ring)],
            "replica", jnp.minimum(r + 1, R - 1),
        )

    def left_copy(c):
        return remote(
            to_l.at[c], from_r.at[c], l_ss.at[lax.rem(c, sends)], l_rs.at[lax.rem(c, left_ring)],
            "replica", jnp.maximum(r - 1, 0),
        )

    def left_cut(i):
        at = pl.ds(i * cut, cut)
        return remote(
            to_l.at[0, at], from_r.at[0, at], l_ss.at[sends + i], l_rs.at[left_ring + i],
            "replica", jnp.maximum(r - 1, 0),
        )

    def send_right(c):
        pl.when(c >= sends)(lambda: right_copy(c - sends).wait_send())
        right_copy(c).start()

    def send_left(c):
        pl.when(c > sends)(lambda: left_copy(c - sends).wait_send())
        left_copy(c).start()

    lane = lax.broadcasted_iota(jnp.int32, (T, HEAD), 1)

    def tables(pos):
        angle = jnp.broadcast_to(pos[...].astype(F32), (T, T)).T[:, :1] * rate[...]
        sine, cosine = sine_cosine(angle)
        return cosine, jnp.where(lane < HEAD // 2, -sine, sine)

    def squares(ref, total, lo, hi):
        for c in range(lo // 128, hi // 128):
            v = ref[:, c * 128 : (c + 1) * 128].astype(F32)
            total = total + v * v
        return total

    def inverse_of(total):
        return lax.rsqrt(jnp.sum(total, -1, keepdims=True) / D + EPS)

    load_posb.wait()
    load_rate.wait()
    cos_b, sin_b = tables(posb_v)
    load_kcot.wait()

    def rotate_back(h):
        for i in range(h * width, (h + 1) * width, HEAD):
            head = slice(i, i + HEAD)
            v = kcot_v[:, head].astype(F32)
            kg_all[0, :, head] = (v * cos_b - pltpu.roll(v, HEAD // 2, 1) * sin_b).astype(BF16)

    rotate_back(0)
    peers = S - 1
    for cond in (s > 0, s < X - 1, r > 0, r < R - 1):
        peers = peers + jnp.where(cond, 1, 0)
    pl.semaphore_wait(barrier, peers)

    def open_exchange():
        for d in range(1, S):
            kg_copy(d, 0).start()
            sv_copy(d, 0).start()

    load_saved[0].wait()
    total = squares(saved_v, jnp.zeros((T, 128), F32), 0, Dl)
    for i in range(1, LOADS):
        load_saved[i].wait()
    pl.when(lax.rem(s, 2) == 0)(open_exchange)
    total = squares(saved_v, total, Dl, D)
    inverse = jnp.broadcast_to(inverse_of(total), (T, 128))
    inv_all[0] = inverse
    inv_row[0] = inverse.T[:8]
    pl.when(lax.rem(s, 2) == 1)(open_exchange)
    for d in range(1, S):
        iv_copy(d).start()
    for h in range(1, PARTS):
        rotate_back(h)
        for d in range(1, S):
            kg_copy(d, h).start()
    for q in range(1, len(pieces)):
        for d in range(1, S):
            sv_copy(d, q).start()
    load_w.start()

    @pl.when(s < X - 1)
    def _():
        for d in (*range(1, S), 0):
            acts_copy(d).start()

    @pl.when(s > 0)
    def _():
        grads_copy.start()

    pl.when(s == 0)(load_acts.start)
    pl.when(s == X - 1)(load_grads.start)
    load_gain.wait()
    load_posf.wait()
    p_acc[...] = jnp.zeros(p_acc.shape, F32)
    sum_v[...] = jnp.zeros(sum_v.shape, F32)

    def rows_of(p):
        o = p * ROWS
        g = gain[:, cols(j, ROWS, o)]
        sides = [saved_v[:, cols(j, ROWS, o)]]
        for d in range(1, S):
            sides.append(sv_recv[d, :, pl.ds(pl.multiple_of(o, 128), ROWS)])
        return jnp.concatenate(
            [(v.astype(F32) * inv_all[d] * g).astype(BF16) for d, v in enumerate(sides)], 0
        )

    def first_term(h):
        at = slice(h * width, (h + 1) * width)
        for d in range(1, S):
            kg_wait(d, h)
        part[h] = lax.dot_general(
            first[...], kg_all[:, :, at].reshape(S * T, width), (((0,), (0,)), ((), ())),
            preferred_element_type=F32,
        )

    def term_of(p):
        for q in range(1, len(pieces)):

            @pl.when(p == pieces[q][0])
            def _():
                for d in range(1, S):
                    sv_wait(d, q)

        term = lax.dot_general(
            rows_of(p), kg_all[...].reshape(S * T, N), (((0,), (0,)), ((), ())),
            preferred_element_type=F32,
        )
        for h in range(PARTS):
            part[p * PARTS + h] = term[:, h * width : (h + 1) * width]

    for d in range(1, S):
        iv_wait(d)
        inv_all[d] = jnp.broadcast_to(inv_row[d][:1], (128, T)).T
        sv_wait(d, 0)
    first[...] = rows_of(0)
    first_term(0)

    def forward_tables():
        cos_f, sin_f = tables(posf_v)
        tab_v[0] = cos_f
        tab_v[1] = sin_f

    def relay():
        pl.when(s == 0)(load_acts.wait)
        for d in range(1, S):
            pl.when(s > 0)(acts_copy(d).wait_recv)
            st_copy(d).start()

    def backward(i):
        pl.when(i == 0)(load_w.wait)
        at = pl.ds(pl.multiple_of(i * tile, 128), tile)
        m = lax.dot_general(
            kg_all[...].reshape(S * T, N), w_v[at, :], (((1,), (1,)), ((), ())),
            preferred_element_type=F32,
        )
        m = (m * gain[:, cols(j, tile, i * tile)]).astype(BF16)
        g_buf[0, :, at] = m[:T]
        for d in range(1, S):
            g_send[d, :, at] = m[d * T : (d + 1) * T]
            g_copy(d, i).start()

    def project(slot, block, i):
        x = (block.astype(F32) * gain[:, cols(j, tile, i * tile)]).astype(BF16)
        at = pl.ds(pl.multiple_of(i * tile, 128), tile)
        p_acc[slot] = p_acc[slot] + jnp.dot(x, w_v[at, :], preferred_element_type=F32)

    def forward_own(i):
        @pl.when((i == 0) & (s > 0))
        def _():
            acts_copy(0).wait_recv()

        project(0, stream_v[:, cols(j, tile, i * tile)], i)

    def forward_peers(i):
        at = pl.ds(pl.multiple_of(i * tile, 128), tile)
        for d in range(1, S):
            @pl.when(i == 0)
            def _():
                st_wait(d)

            project(d, st_recv[d, :, at], i)

            @pl.when(i == tiles - 1)
            def _():
                p_send[d] = p_acc[d].astype(p_send.dtype)
                p_copy(d).start()

    def span_of(q):
        d = q // (Fs // wide)
        return d, lax.rem(q, Fs // wide) * wide

    def grad_means(q):
        @pl.when(q == 0)
        def _():
            for d in range(1, S):
                for i in range(tiles):
                    g_wait(d, i)

        d, o = span_of(q)
        total = sum_v[...]
        for c in range(0, wide, 128):
            v = saved_v[:, cols(peer(d), 128, o + c)].astype(F32)
            total = total + v * g_buf[d, :, pl.ds(pl.multiple_of(o + c, 128), 128)].astype(F32)
        sum_v[...] = total

    def finish_grad(q):
        @pl.when(q == 0)
        def _():
            pl.when(s == X - 1)(load_grads.wait)
            pl.when(s < X - 1)(grads_copy.wait_recv)
            inv = inv_all[0]
            mean = jnp.sum(sum_v[...], -1, keepdims=True) / D
            sum_v[...] = inv * inv * inv * mean

        d, o = span_of(q)
        inv, factor = inv_all[0], sum_v[...]
        for c in range(0, wide, 128):
            at = cols(peer(d), 128, o + c)
            v = saved_v[:, at].astype(F32) * factor
            g = g_buf[d, :, pl.ds(pl.multiple_of(o + c, 128), 128)].astype(F32) * inv
            grad_o[:, at] = (arrived_v[:, at].astype(F32) + g - v).astype(BF16)

    def finish_keys():
        inv = inverse_of(squares(stream_v, jnp.zeros((T, 128), F32), 0, D))
        for d in range(1, S):
            p_wait(d)
        for h in range(N // HEAD):
            head = slice(h * HEAD, (h + 1) * HEAD)
            v = p_acc[0, :, head]
            for d in range(1, S):
                v = v + p_buf[d, :, head].astype(F32)
            v = v * inv
            v = v * tab_v[0] + pltpu.roll(v, HEAD // 2, 1) * tab_v[1]
            keys_o[:, head] = v.astype(BF16)

    scale = float(T * S * R) ** -0.5

    def when_chunk(c, *conds):
        cond = (c >= 0) & (c < C)
        for extra in conds:
            cond = cond & extra
        return pl.when(cond)

    right_lag, left_lag = RIGHT * r, LEFT * (R - 1 - r)
    near, far = jnp.minimum(right_lag, left_lag), jnp.maximum(right_lag, left_lag)
    counts = dict(relay=1, backward=tiles, own=tiles, peers=tiles, means=spans, grads=spans, keys=1)
    start, end = {}, 0
    for name, at in PLAN.items():
        start[name] = max(at * C // SPAN, end)
        end = start[name] + counts[name]
    steps = jnp.maximum(C + far, end)

    def each(t, name, task):
        at = start[name]
        pl.when((t >= at) & (t < at + counts[name]))(lambda: task(t - at))

    def step(t, carry):
        a, b = t - right_lag, t - left_lag

        @pl.when((b == 0) & (r < R - 1))
        def _():
            for i in range(CUTS):
                left_cut(i).wait_recv()
                at = pl.ds(i * cut, cut)

                @pl.when(r > 0)
                def _():
                    to_l[0, at] = (part[0, at] + from_r[0, at].astype(F32)).astype(travel)
                    left_cut(i).start()

        @pl.when((b == 0) & (r == R - 1) & (r > 0))
        def _():
            to_l[0] = part[0].astype(travel)
            for i in range(CUTS):
                left_cut(i).start()

        later = jnp.where(b == 0, -1, b)

        @when_chunk(later, r == R - 1, r > 0)
        def _():
            to_l[b] = part[b].astype(travel)
            send_left(b)

        @when_chunk(a, r == 0, r < R - 1)
        def _():
            to_r[a] = part[a].astype(travel)
            send_right(a)

        @when_chunk(later, r < R - 1)
        def _():
            left_copy(b).wait_recv()

        @when_chunk(later, r < R - 1, r > 0)
        def _():
            to_l[b] = (part[b] + from_r[b].astype(F32)).astype(travel)
            send_left(b)

        @when_chunk(a, r > 0)
        def _():
            right_copy(a).wait_recv()

        @when_chunk(a, r > 0, r < R - 1)
        def _():
            to_r[a] = (part[a] + from_l[a].astype(F32)).astype(travel)
            send_right(a)

        f = t - far

        def finish(*sums):
            rows = pl.ds(pl.multiple_of((f // PARTS) * ROWS, ROWS), ROWS)
            at = pl.ds(pl.multiple_of(lax.rem(f, PARTS) * width, 128), width)
            total = part[f]
            for ref in sums:
                total = total + ref[f].astype(F32)
            wg_o[rows, at] = total * scale

        when_chunk(f, r == 0, r < R - 1)(lambda: finish(from_r))
        when_chunk(f, r > 0, r < R - 1)(lambda: finish(from_l, from_r))
        when_chunk(f, r > 0, r == R - 1)(lambda: finish(from_l))
        if R == 1:
            when_chunk(f)(finish)

        u = t - near
        for h in range(1, PARTS):
            pl.when(u == h - 1)(lambda: first_term(h))
        ahead = u // PARTS + 1

        @pl.when(
            (u >= 0) & (lax.rem(u, PARTS) == jnp.where(u < PARTS, PARTS - 1, 1)) & (ahead < blocks)
        )
        def _():
            term_of(ahead)

        pl.when(t == PARTS)(forward_tables)
        pl.when(t == start["relay"])(relay)
        each(t, "backward", backward)
        each(t, "own", forward_own)
        each(t, "peers", forward_peers)
        each(t, "means", grad_means)
        each(t, "grads", finish_grad)
        pl.when(t == start["keys"])(finish_keys)
        return carry

    lax.fori_loop(0, steps, step, 0)

    for d in range(1, S):
        for q in range(len(pieces)):
            sv_copy(d, q).wait_send()
        for h in range(PARTS):
            kg_copy(d, h).wait_send()
        iv_copy(d).wait_send()
        st_copy(d).wait_send()
        for i in range(tiles):
            g_copy(d, i).wait_send()
        p_copy(d).wait_send()

    @pl.when(s < X - 1)
    def _():
        for d in range(S):
            acts_copy(d).wait_send()

    @pl.when(s > 0)
    def _():
        grads_copy.wait_send()

    @pl.when(r < R - 1)
    def _():
        for c in range(C - sends, C):
            right_copy(c).wait_send()

    @pl.when(r > 0)
    def _():
        for i in range(CUTS):
            left_cut(i).wait_send()
        for c in range(max(C - sends, 1), C):
            left_copy(c).wait_send()


def store_kernel(a, b, c, a_out, b_out, c_out, sem):
    copies = [
        pltpu.make_async_copy(src, dst, sem.at[i])
        for i, (src, dst) in enumerate(((c, c_out), (b, b_out), (a, a_out)))
    ]
    for copy in copies:
        copy.start()
    for copy in copies:
        copy.wait()


def per_device(acts_fwd, pos_fwd, saved_acts, pos_bwd, grads_in, key_cotan, weight, gain):
    X, S, R = (lax.axis_size(a) for a in ("section", "shard", "replica"))
    T, D = acts_fwd.shape[1:]
    Fs, N = weight.shape[1:]
    C = Fs // ROWS * PARTS
    width = N // PARTS
    pieces = len(pieces_of(Fs // ROWS))
    sends, right_ring, left_ring = rings(C, R)
    others = max(S - 1, 1)
    tiles = Fs // min(512, Fs)
    travel = BF16 if R <= 8 else F32
    index = np.arange(HEAD) % (HEAD // 2)
    rate = jnp.asarray(THETA ** (-(2.0 * index) / HEAD), F32)[None]
    hbm = pl.BlockSpec(memory_space=pltpu.HBM)
    vmem = pl.BlockSpec(memory_space=pltpu.VMEM)
    dma = pltpu.SemaphoreType.DMA
    results = pl.pallas_call(
        functools.partial(kernel, X, S, R),
        out_shape=(
            pltpu.VMEM((T, N), BF16),
            pltpu.VMEM((T, D), BF16),
            pltpu.VMEM((Fs, N), F32),
        ),
        in_specs=[hbm] * 9,
        out_specs=(vmem, vmem, vmem),
        scratch_shapes=[
            pltpu.VMEM((T, D), BF16),
            pltpu.VMEM((T, N), BF16),
            pltpu.VMEM((Fs, N), BF16),
            pltpu.VMEM((T, D), BF16),
            pltpu.VMEM((T, D), BF16),
            pltpu.VMEM((1, D), F32),
            pltpu.VMEM((1, T), jnp.int32),
            pltpu.VMEM((1, T), jnp.int32),
            pltpu.VMEM((1, HEAD), F32),
            pltpu.VMEM((S, T, Fs), BF16),
            pltpu.VMEM((S, T, N), BF16),
            pltpu.VMEM((S, T, Fs), BF16),
            pltpu.VMEM((S, T, Fs), BF16),
            pltpu.VMEM((S, T, Fs), BF16),
            pltpu.VMEM((S, T, N), BF16),
            pltpu.VMEM((S, T, N), BF16),
            pltpu.VMEM((S, T, N), F32),
            pltpu.VMEM((C, ROWS, width), F32),
            pltpu.VMEM((C, ROWS, width), travel),
            pltpu.VMEM((C, ROWS, width), travel),
            pltpu.VMEM((C, ROWS, width), travel),
            pltpu.VMEM((C, ROWS, width), travel),
            pltpu.VMEM((S, T, 128), F32),
            pltpu.VMEM((S, 8, T), F32),
            pltpu.VMEM((2, T, HEAD), F32),
            pltpu.VMEM((T, 128), F32),
            pltpu.VMEM((S * T, ROWS), BF16),
            dma((5,)), dma((LOADS,)),
            dma((S,)), dma((S,)), dma((2,)),
            dma((others, pieces)), dma((others, pieces)),
            dma((others, PARTS)), dma((others, PARTS)),
            dma((others,)), dma((others,)),
            dma((others,)), dma((others,)),
            dma((others, tiles)), dma((others, tiles)),
            dma((others,)), dma((others,)),
            dma((sends,)), dma((right_ring,)), dma((sends + CUTS,)), dma((left_ring + CUTS,)),
        ],
        compiler_params=pltpu.CompilerParams(
            collective_id=0, has_side_effects=True, vmem_limit_bytes=int(57.8 * 2**20)
        ),
        name="relay_window",
    )(
        acts_fwd[0], grads_in[0], saved_acts[0], key_cotan[0], weight[0],
        gain, pos_fwd, pos_bwd, rate,
    )
    keys, grad_out, weight_grad = pl.pallas_call(
        store_kernel,
        out_shape=tuple(jax.ShapeDtypeStruct(v.shape, v.dtype) for v in results),
        in_specs=[vmem] * 3,
        out_specs=[hbm] * 3,
        scratch_shapes=[dma((3,))],
        compiler_params=pltpu.CompilerParams(vmem_limit_bytes=8 * 2**20),
        name="store_results",
    )(*results)
    return keys[None], grad_out[None], weight_grad[None]


def solution(mesh):
    placed = (
        P("section", ("shard", "replica"), None),
        P("section", ("shard", "replica")),
        P("section", ("shard", "replica"), None),
        P("section", ("shard", "replica")),
        P("section", ("shard", "replica"), None),
        P("section", ("shard", "replica"), None),
        P("section", "shard", None),
        P("section", None),
    )
    return jax.shard_map(
        per_device,
        mesh=mesh,
        in_specs=placed,
        out_specs=(
            P("section", ("shard", "replica"), None),
            P("section", ("shard", "replica"), None),
            P("section", "shard", None),
        ),
        check_vma=False,
    )
```
